32 devices in a mesh: rep: 4 (over y, core), grp: 8 (over z, x).
Axes of the slice: x: 2, y: 2, z: 4, core: 2. Of those that a mesh axis runs over, the one named last changes fastest.
Arguments:
- hidden_in: bfloat16 [128, 7168], P(('rep', 'grp')), may hold values from -3 to 3
- q_nope: bfloat16 [128, 8192], P(('rep', 'grp')), may hold values from -9 to 9
- q_rope: bfloat16 [128, 4096], P(('rep', 'grp')), may hold values from -36 to 36
- new_kv: bfloat16 [128, 576], P(('rep', 'grp')), may hold values from -6 to 6
- cache_kv: bfloat16 [128, 4096, 576], P(('rep', 'grp')), may hold values from -10 to 10
- lengths: int32 [128], P(('rep', 'grp')), may hold values from 2 to 4096, as said below
- w_uk: bfloat16 [512, 8192], P('rep'), may hold values from -0.5 to 0.5
- w_uv: bfloat16 [512, 8192], P('rep'), may hold values from -0.25 to 0.25
- w_out: bfloat16 [8192, 7168], P('grp'), may hold values from -0.0625 to 0.0625
- norm_gain: bfloat16 [7168], replicated, may hold values from 0.5 to 1.5
- w_gate: bfloat16 [7168, 18432], P(None, ('rep', 'grp')), may hold values from -0.0625 to 0.0625
- w_up: bfloat16 [7168, 18432], P(None, ('rep', 'grp')), may hold values from -0.0625 to 0.0625
- w_down: bfloat16 [18432, 7168], P(('rep', 'grp')), may hold values from -0.046875 to 0.046875
Outputs:
- hidden_out: bfloat16 [128, 7168], P(('rep', 'grp'))
The draws below stay inside these ranges and needn't reach their ends.
Inputs may be any that keep to these rules, and one draw needn't show every extreme that they name: `lengths`: every sequence has 2 or more cached positions and at most 4096; some sequence has exactly 4096.
All inputs are finite; a program needn't handle non-finite values.
Results may differ from the reference program's by a relative error of at most 0.03.
Values may be sent and summed in bfloat16 or wider, within the bound.
A program may use at most 192 MiB of HBM per device.

```python
import jax
import jax.numpy as jnp
from jax import lax

D = 7168
FF = 18432
H = 64
NOPE = 128
ROPE = 64
VH = 128
KV_RANK = 512
CACHE = 4096
SEQS = 128


def draw_q_rope(key, part):
    values = jnp.clip(jax.random.normal(jax.random.fold_in(key, 3), (SEQS, H, ROPE), jnp.float32), -6.0, 6.0)
    return values.reshape(SEQS, H * ROPE).astype(jnp.bfloat16)


def draw_cache_kv(key, part):
    inner = jax.random.fold_in(key, 4)
    values = jnp.clip(jax.random.normal(inner, (SEQS, CACHE, KV_RANK + ROPE), jnp.float32), -6.0, 6.0)
    return values.astype(jnp.bfloat16)


def draw_lengths(key, part):
    inner = jax.random.fold_in(key, 5)
    lengths_drawn = jax.random.randint(inner, (SEQS,), 2, CACHE + 1, dtype=jnp.int32)
    where_full = jax.random.randint(jax.random.fold_in(inner, 6), (), 0, SEQS, dtype=jnp.int32)
    return jnp.where(jnp.arange(SEQS, dtype=jnp.int32) == where_full, CACHE, lengths_drawn).astype(jnp.int32)


def block_levels(key, shape, split, smallest, high):
    def one(position, shards_of):
        steps = jax.random.uniform(jax.random.fold_in(jax.random.fold_in(key, 6), position), (shards_of,), jnp.float32, smallest / len(split), high / len(split))
        return jnp.repeat(jnp.exp(steps), shape[position] // shards_of).reshape((-1,) + (1,) * (len(shape) - position - 1))

    loudness = one(*split[0])
    for cut in split[1:]:
        loudness = loudness * one(*cut)
    return loudness


def normal_values(stream_key, extent, scale, bound, pieces=(), kind=jnp.bfloat16):
    array = jax.random.normal(stream_key, extent, jnp.float32) * scale
    if len(pieces) > 0:
        array = block_levels(stream_key, extent, pieces, -0.22, 0.18) * array
    return jnp.clip(array, min=-bound, max=bound).astype(kind)


def setup_inputs(seed: int = 0) -> dict:
    key_list = jax.random.split(jax.random.key(seed), 14)
    return {
        "hidden_in": normal_values(key_list[0], (SEQS, D), 0.5, 3.0, ((0, 32),)),
        "q_nope": normal_values(key_list[1], (SEQS, H * NOPE), 1.5, 9.0, ((0, 32),)),
        "q_rope": draw_q_rope(jax.random.fold_in(key_list[13], 71), 0),
        "new_kv": normal_values(key_list[3], (SEQS, KV_RANK + ROPE), 1.0, 6.0, ((0, 32),)),
        "cache_kv": draw_cache_kv(jax.random.fold_in(key_list[13], 71), 0),
        "lengths": draw_lengths(jax.random.fold_in(key_list[13], 71), 0),
        "w_uk": normal_values(key_list[6], (KV_RANK, H * NOPE), NOPE ** -0.5, 0.5, ((0, 4),)),
        "w_uv": normal_values(key_list[7], (KV_RANK, H * VH), KV_RANK ** -0.5, 0.25, ((0, 4),)),
        "w_out": normal_values(key_list[8], (H * VH, D), (H * VH) ** -0.5, 0.0625, ((0, 8),)),
        "norm_gain": jnp.clip(1.0 + 0.1 * jax.random.normal(key_list[9], (D,), jnp.float32), 0.5, 1.5).astype(jnp.bfloat16),
        "w_gate": normal_values(key_list[10], (D, FF), D ** -0.5, 0.0625, ((1, 32),)),
        "w_up": normal_values(key_list[11], (D, FF), D ** -0.5, 0.0625, ((1, 32),)),
        "w_down": normal_values(key_list[12], (FF, D), FF ** -0.5, 0.046875, ((0, 32),)),
    }


epsilon = 1e-06

def norm_rows(resid, norm_gain):
    resid_f32 = resid.astype(jnp.float32)
    mean_sq = lax.optimization_barrier(jnp.mean(resid_f32 * resid_f32, axis=1, keepdims=True))
    return (resid_f32 * lax.rsqrt(mean_sq + epsilon) * norm_gain.astype(jnp.float32)).astype(jnp.bfloat16)

def reference(hidden_in, q_nope, q_rope, new_kv, cache_kv, lengths, w_uk, w_uv, w_out, norm_gain, w_gate, w_up, w_down):
    seq_count = hidden_in.shape[0]
    nope_part = q_nope.reshape(seq_count, H, NOPE).astype(jnp.float32)
    key_up = w_uk.reshape(KV_RANK, H, NOPE).astype(jnp.float32)
    q_lat = jnp.einsum('bhd,chd->bhc', nope_part, key_up).astype(jnp.bfloat16)
    queries = jnp.concatenate([q_lat, q_rope.reshape(seq_count, H, ROPE)], axis=2)
    score_scale = float(NOPE + ROPE) ** (-0.5)
    positions = jnp.arange(CACHE, dtype=jnp.int32)

    def attend(sequence_item):
        one_query, one_cache, one_new, one_length = sequence_item
        scores = jnp.dot(one_query, one_cache.T, preferred_element_type=jnp.float32) * score_scale
        scores = jnp.where(positions[None, :] < one_length, scores, -jnp.inf)
        own_score = jnp.dot(one_query, one_new, preferred_element_type=jnp.float32) * score_scale
        row_top = jnp.maximum(lax.optimization_barrier(jnp.max(scores, axis=1)), own_score)
        weights = jnp.exp(scores - row_top[:, None])
        own_weight = jnp.exp(own_score - row_top)
        denom_sum = lax.optimization_barrier(jnp.sum(weights, axis=1)) + own_weight
        softmax_w = (weights / denom_sum[:, None]).astype(jnp.bfloat16)
        own_prob = (own_weight / denom_sum).astype(jnp.bfloat16)
        mixture = jnp.dot(softmax_w, one_cache, preferred_element_type=jnp.float32)
        mixture = mixture + own_prob.astype(jnp.float32)[:, None] * one_new.astype(jnp.float32)[None, :]
        return mixture[:, :KV_RANK].astype(jnp.bfloat16)
    latent = lax.map(attend, (queries, cache_kv, new_kv, lengths))
    value_up = w_uv.reshape(KV_RANK, H, VH).astype(jnp.float32)
    head_out = jnp.einsum('bhc,che->bhe', latent.astype(jnp.float32), value_up).astype(jnp.bfloat16)
    attn_out = jnp.dot(head_out.reshape(seq_count, H * VH), w_out, preferred_element_type=jnp.float32)
    resid = (hidden_in.astype(jnp.float32) + attn_out).astype(jnp.bfloat16)
    normed = norm_rows(resid, norm_gain)
    gate_val = jnp.dot(normed, w_gate, preferred_element_type=jnp.float32)
    up_val = jnp.dot(normed, w_up, preferred_element_type=jnp.float32)
    activated = (jax.nn.silu(gate_val) * up_val).astype(jnp.bfloat16)
    mlp_out = jnp.dot(activated, w_down, preferred_element_type=jnp.float32)
    return (resid.astype(jnp.float32) + mlp_out).astype(jnp.bfloat16)
```

```python
import functools

import jax
import jax.numpy as jnp
from jax import lax
from jax.experimental import pallas as pl
from jax.experimental.pallas import tpu as pltpu
from jax.sharding import PartitionSpec as P

H = 64
NOPE = 128
ROPE = 64
VH = 128
KV_RANK = 512
CACHE = 4096
MESH = pl.DeviceIdType.MESH

epsilon = 1e-06


def _exchange_kernel(axis, n, gather, x_ref, out_ref, send_sem, recv_sem, own_sem):
    me = lax.axis_index(axis)
    barrier = pltpu.get_barrier_semaphore()

    def greet(k, carry):
        peer = lax.rem(me + k, n)
        pl.semaphore_signal(barrier, inc=1, device_id={axis: peer}, device_id_type=MESH)
        return carry

    lax.fori_loop(1, n, greet, 0)
    own = pltpu.make_async_copy(x_ref if gather else x_ref.at[me], out_ref.at[me], own_sem)
    own.start()
    pl.semaphore_wait(barrier, n - 1)

    def send(k, carry):
        peer = lax.rem(me + k, n)
        pltpu.make_async_remote_copy(
            src_ref=x_ref if gather else x_ref.at[peer],
            dst_ref=out_ref.at[me],
            send_sem=send_sem.at[k - 1],
            recv_sem=recv_sem.at[k - 1],
            device_id={axis: peer},
            device_id_type=MESH,
        ).start()
        return carry

    lax.fori_loop(1, n, send, 0)
    own.wait()

    def finish(k, carry):
        source = lax.rem(me + n - k, n)
        peer = lax.rem(me + k, n)
        pltpu.make_async_remote_copy(
            src_ref=x_ref if gather else x_ref.at[peer],
            dst_ref=out_ref.at[source],
            send_sem=send_sem.at[k - 1],
            recv_sem=recv_sem.at[k - 1],
            device_id={axis: peer},
            device_id_type=MESH,
        ).wait()
        return carry

    lax.fori_loop(1, n, finish, 0)


def exchange(x, axis, n, gather, cid):
    out_shape = ((n,) + x.shape) if gather else x.shape
    return pl.pallas_call(
        functools.partial(_exchange_kernel, axis, n, gather),
        out_shape=jax.ShapeDtypeStruct(out_shape, x.dtype),
        in_specs=[pl.BlockSpec(memory_space=pltpu.VMEM)],
        out_specs=pl.BlockSpec(memory_space=pltpu.VMEM),
        scratch_shapes=[
            pltpu.SemaphoreType.DMA((n - 1,)),
            pltpu.SemaphoreType.DMA((n - 1,)),
            pltpu.SemaphoreType.DMA,
        ],
        compiler_params=pltpu.CompilerParams(collective_id=cid, has_side_effects=True),
    )(x)


def _chip_facts(group):
    rep = lax.axis_index("rep")
    grp = lax.axis_index("grp")
    core = lax.rem(rep, 2)
    chip = lax.div(rep, 2) * group + grp
    partner = {"rep": rep + 1 - 2 * core}

    def device(c):
        return {"rep": lax.div(c, group) * 2 + core, "grp": lax.rem(c, group)}

    def block(c, k):
        return (lax.div(c, group) * 2 + k) * group + lax.rem(c, group)

    return core, chip, partner, device, block


def _greet_chips(chips, chip, partner, device):
    barrier = pltpu.get_barrier_semaphore()
    pl.semaphore_signal(barrier, inc=1, device_id=partner, device_id_type=MESH)

    def greet(k, carry):
        pl.semaphore_signal(
            barrier, inc=1, device_id=device(lax.rem(chip + k, chips)), device_id_type=MESH
        )
        return carry

    lax.fori_loop(1, chips, greet, 0)
    return barrier


def _gather_all_kernel(chips, group, x_ref, out_ref, send_sem, recv_sem, send2, recv2, own_sem):
    core, chip, partner, device, block = _chip_facts(group)
    barrier = _greet_chips(chips, chip, partner, device)
    mine = block(chip, core)
    own = pltpu.make_async_copy(x_ref, out_ref.at[mine], own_sem)
    own.start()
    pl.semaphore_wait(barrier, chips)

    def across(k, slot):
        return pltpu.make_async_remote_copy(
            src_ref=x_ref,
            dst_ref=out_ref.at[slot],
            send_sem=send_sem.at[k],
            recv_sem=recv_sem.at[k],
            device_id=device(lax.rem(chip + k, chips)),
            device_id_type=MESH,
        )

    def relay(k, slot):
        return pltpu.make_async_remote_copy(
            src_ref=out_ref.at[slot],
            dst_ref=out_ref.at[slot],
            send_sem=send2.at[k],
            recv_sem=recv2.at[k],
            device_id=partner,
            device_id_type=MESH,
        )

    def send(k, carry):
        across(k, mine).start()
        return carry

    lax.fori_loop(1, chips, send, 0)
    own.wait()
    relay(0, mine).start()

    def forward(k, carry):
        slot = block(lax.rem(chip + chips - k, chips), core)
        across(k, slot).wait_recv()
        relay(k, slot).start()
        return carry

    lax.fori_loop(1, chips, forward, 0)

    def finish(k, carry):
        source = lax.rem(chip + chips - k, chips)
        relay(k, block(source, 1 - core)).wait_recv()
        relay(k, block(source, core)).wait_send()
        return carry

    lax.fori_loop(0, chips, finish, 0)

    def drain(k, carry):
        across(k, mine).wait_send()
        return carry

    lax.fori_loop(1, chips, drain, 0)


def gather_all(x, rep_count, group, cid):
    chips = rep_count // 2 * group
    return pl.pallas_call(
        functools.partial(_gather_all_kernel, chips, group),
        out_shape=jax.ShapeDtypeStruct((rep_count * group,) + x.shape, x.dtype),
        in_specs=[pl.BlockSpec(memory_space=pltpu.VMEM)],
        out_specs=pl.BlockSpec(memory_space=pltpu.VMEM),
        scratch_shapes=[pltpu.SemaphoreType.DMA((chips,))] * 4 + [pltpu.SemaphoreType.DMA],
        compiler_params=pltpu.CompilerParams(collective_id=cid, has_side_effects=True),
    )(x)


def _reduce_all_kernel(
    chips, group, x_ref, base_ref, out_ref, pair_buf, send_buf, land, send1, recv1, send2, recv2
):
    core, chip, partner, device, block = _chip_facts(group)
    barrier = _greet_chips(chips, chip, partner, device)
    pl.semaphore_wait(barrier, chips)

    def to_partner(k):
        target = lax.rem(chip + k, chips)
        return pltpu.make_async_remote_copy(
            src_ref=x_ref.at[block(target, 1 - core)],
            dst_ref=pair_buf.at[k],
            send_sem=send1.at[k],
            recv_sem=recv1.at[k],
            device_id=partner,
            device_id_type=MESH,
        )

    def across(k):
        return pltpu.make_async_remote_copy(
            src_ref=send_buf.at[k],
            dst_ref=land.at[k],
            send_sem=send2.at[k],
            recv_sem=recv2.at[k],
            device_id=device(lax.rem(chip + k, chips)),
            device_id_type=MESH,
        )

    def start_pair(i, carry):
        to_partner(lax.rem(i, chips)).start()
        return carry

    lax.fori_loop(1, chips + 1, start_pair, 0)

    def add_pair(k, carry):
        to_partner(k).wait_recv()
        target = lax.rem(chip + k, chips)
        total = x_ref[block(target, core)].astype(jnp.float32) + pair_buf[k].astype(jnp.float32)
        send_buf[k] = total.astype(send_buf.dtype)

        @pl.when(k > 1)
        def _():
            across(k - 1).start()

        return carry

    lax.fori_loop(1, chips, add_pair, 0)
    to_partner(0).wait_recv()
    across(chips - 1).start()
    out_ref[...] = (
        base_ref[...].astype(jnp.float32)
        + x_ref[block(chip, core)].astype(jnp.float32)
        + pair_buf[0].astype(jnp.float32)
    )

    def take(k, carry):
        across(k).wait_recv()
        out_ref[...] += land[k].astype(jnp.float32)
        return carry

    lax.fori_loop(1, chips, take, 0)

    def drain(k, carry):
        to_partner(k).wait_send()

        @pl.when(k > 0)
        def _():
            across(k).wait_send()

        return carry

    lax.fori_loop(0, chips, drain, 0)


def reduce_all(x, base, rep_count, group, cid):
    chips = rep_count // 2 * group
    piece = x.shape[1:]
    return pl.pallas_call(
        functools.partial(_reduce_all_kernel, chips, group),
        out_shape=jax.ShapeDtypeStruct(piece, jnp.float32),
        in_specs=[pl.BlockSpec(memory_space=pltpu.VMEM)] * 2,
        out_specs=pl.BlockSpec(memory_space=pltpu.VMEM),
        scratch_shapes=[
            pltpu.VMEM((chips,) + piece, x.dtype),
            pltpu.VMEM((chips,) + piece, x.dtype),
            pltpu.VMEM((chips,) + piece, x.dtype),
        ]
        + [pltpu.SemaphoreType.DMA((chips,))] * 4,
        compiler_params=pltpu.CompilerParams(collective_id=cid, has_side_effects=True),
    )(x, base)


def norm_rows(resid, norm_gain):
    resid_f32 = resid.astype(jnp.float32)
    mean_sq = jnp.mean(resid_f32 * resid_f32, axis=1, keepdims=True)
    return (resid_f32 * lax.rsqrt(mean_sq + epsilon) * norm_gain.astype(jnp.float32)).astype(
        jnp.bfloat16
    )


def gated_rows(rows_in, gate_cols, up_cols):
    gate_val = jnp.dot(rows_in, gate_cols, preferred_element_type=jnp.float32)
    up_val = jnp.dot(rows_in, up_cols, preferred_element_type=jnp.float32)
    return (jax.nn.silu(gate_val) * up_val).astype(jnp.bfloat16)


def on_device(
    rep_count,
    group,
    hidden_in,
    q_nope,
    q_rope,
    new_kv,
    cache_kv,
    lengths,
    w_uk,
    w_uv,
    w_out,
    norm_gain,
    w_gate,
    w_up,
    w_down,
):
    seq_count = hidden_in.shape[0]
    heads_here = H // group
    slice_width = w_uk.shape[0]
    grp = lax.axis_index("grp")
    rep = lax.axis_index("rep")

    uv_own = lax.dynamic_slice_in_dim(w_uv, grp * heads_here * VH, heads_here * VH, 1)
    uv_parts = jnp.zeros((rep_count,) + uv_own.shape, uv_own.dtype)
    uv_parts = lax.dynamic_update_slice_in_dim(uv_parts, uv_own[None], rep, 0)
    for step in range(1, rep_count):
        moved = lax.ppermute(
            uv_own, "rep", [(i, (i + step) % rep_count) for i in range(rep_count)]
        )
        source = lax.rem(rep + rep_count - step, rep_count)
        uv_parts = lax.dynamic_update_slice_in_dim(uv_parts, moved[None], source, 0)
    value_up = uv_parts.reshape(KV_RANK, heads_here, VH)

    q_rows = exchange(q_nope.reshape(seq_count * H, NOPE), "rep", rep_count, True, 1)
    q_part = jnp.einsum(
        "bhd,chd->bhc",
        q_rows.reshape(rep_count * seq_count, H, NOPE),
        w_uk.reshape(slice_width, H, NOPE),
        preferred_element_type=jnp.float32,
    ).astype(jnp.bfloat16)
    q_back = exchange(
        q_part.reshape(rep_count, seq_count * H, slice_width), "rep", rep_count, False, 2
    )
    q_lat = q_back.reshape(rep_count, seq_count, H, slice_width)
    queries = jnp.concatenate(
        [q_lat[i] for i in range(rep_count)] + [q_rope.reshape(seq_count, H, ROPE)], axis=2
    )
    score_scale = float(NOPE + ROPE) ** (-0.5)
    scores = (
        jnp.einsum("bhc,blc->bhl", queries, cache_kv, preferred_element_type=jnp.float32)
        * score_scale
    )
    positions = lax.broadcasted_iota(jnp.int32, (1, 1, CACHE), 2)
    scores = jnp.where(positions < lengths[:, None, None], scores, -jnp.inf)
    own_score = (
        jnp.einsum("bhc,bc->bh", queries, new_kv, preferred_element_type=jnp.float32) * score_scale
    )
    row_top = jnp.maximum(jnp.max(scores, axis=2), own_score)
    weights = jnp.exp(scores - row_top[:, :, None])
    own_weight = jnp.exp(own_score - row_top)
    denom_sum = jnp.sum(weights, axis=2) + own_weight
    softmax_w = (weights / denom_sum[:, :, None]).astype(jnp.bfloat16)
    own_prob = (own_weight / denom_sum).astype(jnp.bfloat16)
    mixture = jnp.einsum("bhl,blc->bhc", softmax_w, cache_kv, preferred_element_type=jnp.float32)
    mixture = (
        mixture + own_prob.astype(jnp.float32)[:, :, None] * new_kv.astype(jnp.float32)[:, None, :]
    )
    latent = mixture[:, :, :KV_RANK].astype(jnp.bfloat16)

    by_heads = latent.reshape(seq_count, group, heads_here, KV_RANK).transpose(1, 0, 2, 3)
    latent_here = exchange(
        by_heads.reshape(group, seq_count * heads_here, KV_RANK), "grp", group, False, 3
    ).reshape(group * seq_count, heads_here, KV_RANK)
    head_out = jnp.einsum(
        "bhc,che->bhe", latent_here, value_up, preferred_element_type=jnp.float32
    ).astype(jnp.bfloat16)
    partial_value = jnp.dot(
        head_out.reshape(group * seq_count, heads_here * VH),
        w_out,
        preferred_element_type=jnp.float32,
    ).astype(jnp.bfloat16)
    pieces = exchange(
        partial_value.reshape(group, seq_count, partial_value.shape[1]), "grp", group, False, 4
    )
    resid_own = (
        hidden_in.astype(jnp.float32) + jnp.sum(pieces.astype(jnp.float32), axis=0)
    ).astype(jnp.bfloat16)
    normed = norm_rows(resid_own, norm_gain)
    every_row = gather_all(normed, rep_count, group, 5)
    every_row = every_row.reshape(rep_count * group * seq_count, -1)
    activated = gated_rows(every_row, w_gate, w_up)
    mlp_part = jnp.dot(activated, w_down, preferred_element_type=jnp.float32).astype(jnp.bfloat16)
    total = reduce_all(
        mlp_part.reshape(rep_count * group, seq_count, -1), resid_own, rep_count, group, 6
    )
    return total.astype(jnp.bfloat16)


def solution(mesh):
    return jax.shard_map(
        functools.partial(on_device, mesh.shape["rep"], mesh.shape["grp"]),
        mesh=mesh,
        in_specs=(
            P(("rep", "grp"), None),
            P(("rep", "grp"), None),
            P(("rep", "grp"), None),
            P(("rep", "grp"), None),
            P(("rep", "grp"), None, None),
            P(("rep", "grp")),
            P("rep", None),
            P("rep", None),
            P("grp", None),
            P(),
            P(None, ("rep", "grp")),
            P(None, ("rep", "grp")),
            P(("rep", "grp"), None),
        ),
        out_specs=P(("rep", "grp"), None),
        check_vma=False,
    )
```

```python
import functools

import jax
import jax.numpy as jnp
from jax import lax
from jax.experimental import pallas as pl
from jax.experimental.pallas import tpu as pltpu
from jax.sharding import PartitionSpec as P

H = 64
NOPE = 128
ROPE = 64
VH = 128
KV_RANK = 512
CACHE = 4096
MESH = pl.DeviceIdType.MESH

epsilon = 1e-06


def _exchange_kernel(axis, n, gather, x_ref, out_ref, send_sem, recv_sem, own_sem):
    me = lax.axis_index(axis)
    barrier = pltpu.get_barrier_semaphore()

    def greet(k, carry):
        peer = lax.rem(me + k, n)
        pl.semaphore_signal(barrier, inc=1, device_id={axis: peer}, device_id_type=MESH)
        return carry

    lax.fori_loop(1, n, greet, 0)
    own = pltpu.make_async_copy(x_ref if gather else x_ref.at[me], out_ref.at[me], own_sem)
    own.start()
    pl.semaphore_wait(barrier, n - 1)

    def send(k, carry):
        peer = lax.rem(me + k, n)
        pltpu.make_async_remote_copy(
            src_ref=x_ref if gather else x_ref.at[peer],
            dst_ref=out_ref.at[me],
            send_sem=send_sem.at[k - 1],
            recv_sem=recv_sem.at[k - 1],
            device_id={axis: peer},
            device_id_type=MESH,
        ).start()
        return carry

    lax.fori_loop(1, n, send, 0)
    own.wait()

    def finish(k, carry):
        source = lax.rem(me + n - k, n)
        peer = lax.rem(me + k, n)
        pltpu.make_async_remote_copy(
            src_ref=x_ref if gather else x_ref.at[peer],
            dst_ref=out_ref.at[source],
            send_sem=send_sem.at[k - 1],
            recv_sem=recv_sem.at[k - 1],
            device_id={axis: peer},
            device_id_type=MESH,
        ).wait()
        return carry

    lax.fori_loop(1, n, finish, 0)


def exchange(x, axis, n, gather, cid):
    out_shape = ((n,) + x.shape) if gather else x.shape
    return pl.pallas_call(
        functools.partial(_exchange_kernel, axis, n, gather),
        out_shape=jax.ShapeDtypeStruct(out_shape, x.dtype),
        in_specs=[pl.BlockSpec(memory_space=pltpu.VMEM)],
        out_specs=pl.BlockSpec(memory_space=pltpu.VMEM),
        scratch_shapes=[
            pltpu.SemaphoreType.DMA((n - 1,)),
            pltpu.SemaphoreType.DMA((n - 1,)),
            pltpu.SemaphoreType.DMA,
        ],
        compiler_params=pltpu.CompilerParams(collective_id=cid, has_side_effects=True),
    )(x)


def _pair_kernel(h_ref, r_ref, h_out, r_out, send_sem, recv_sem, own_sem):
    rep = lax.axis_index("rep")
    core = lax.rem(rep, 2)
    partner = {"rep": rep + 1 - 2 * core}
    barrier = pltpu.get_barrier_semaphore()
    pl.semaphore_signal(barrier, inc=1, device_id=partner, device_id_type=MESH)
    own = [
        pltpu.make_async_copy(src, dst.at[core], own_sem.at[i])
        for i, (src, dst) in enumerate(((h_ref, h_out), (r_ref, r_out)))
    ]
    for copy in own:
        copy.start()
    pl.semaphore_wait(barrier, 1)

    def remote(i, src, dst, slot):
        return pltpu.make_async_remote_copy(
            src_ref=src,
            dst_ref=dst.at[slot],
            send_sem=send_sem.at[i],
            recv_sem=recv_sem.at[i],
            device_id=partner,
            device_id_type=MESH,
        )

    remote(0, h_ref, h_out, core).start()
    remote(1, r_ref, r_out, core).start()
    for copy in own:
        copy.wait()
    remote(0, h_ref, h_out, 1 - core).wait()
    remote(1, r_ref, r_out, 1 - core).wait()


def pair_gather(heads, resid, cid):
    vmem = pl.BlockSpec(memory_space=pltpu.VMEM)
    return pl.pallas_call(
        _pair_kernel,
        out_shape=[jax.ShapeDtypeStruct((2,) + v.shape, v.dtype) for v in (heads, resid)],
        in_specs=[vmem] * 2,
        out_specs=[vmem] * 2,
        scratch_shapes=[pltpu.SemaphoreType.DMA((2,))] * 3,
        compiler_params=pltpu.CompilerParams(collective_id=cid, has_side_effects=True),
    )(heads, resid)


def _half_product_kernel(core_ref, x_ref, w_ref, out_ref):
    out_ref[...] = jnp.dot(x_ref[...], w_ref[...], preferred_element_type=jnp.float32).astype(
        out_ref.dtype
    )


def half_product(core, x, w):
    rows, depth = x.shape
    half = w.shape[1] // 2
    tile = half // 7
    return pl.pallas_call(
        _half_product_kernel,
        out_shape=jax.ShapeDtypeStruct((rows, half), x.dtype),
        grid_spec=pltpu.PrefetchScalarGridSpec(
            num_scalar_prefetch=1,
            grid=(7,),
            in_specs=[
                pl.BlockSpec((rows, depth), lambda i, core: (0, 0)),
                pl.BlockSpec((depth, tile), lambda i, core: (0, core[0] * 7 + i)),
            ],
            out_specs=pl.BlockSpec((rows, tile), lambda i, core: (0, i)),
        ),
    )(core, x, w)


def _mlp_kernel(
    zs,
    part,
    hid,
    gain,
    wg_hbm,
    wu_hbm,
    wd_hbm,
    out,
    wg,
    wu,
    wd,
    ra,
    sz,
    rz,
    ssq_out,
    ssq_in,
    rows,
    acc_g,
    acc_u,
    act,
    pout,
    pin,
    own,
    sb,
    rb,
    sa2,
    ra2,
    sz2,
    rz2,
    resid,
    w_sem,
    a_s,
    a_r,
    z_s,
    z_r,
    q_s,
    q_r,
    gz_s,
    gz_r,
    ga_s,
    ga_r,
    gb_s,
    gb_r,
    gp_s,
    gp_r,
    t_s,
    t_r,
    b2_s,
    b2_r,
    a2_s,
    a2_r,
    z2_s,
    z2_r,
    f_s,
    f_r,
):
    rep = lax.axis_index("rep")
    grp = lax.axis_index("grp")
    core = lax.rem(rep, 2)
    y = lax.div(rep, 2)
    z = lax.div(grp, 2)
    x = lax.rem(grp, 2)
    half = part.shape[2]
    tile = half // 7
    own_cols = pl.ds(pl.multiple_of(core * half, 128), half)
    far_cols = pl.ds(pl.multiple_of((1 - core) * half, 128), half)
    f32 = jnp.float32

    weights = [
        pltpu.make_async_copy(src, dst, w_sem.at[i])
        for i, (src, dst) in enumerate(((wg_hbm, wg), (wu_hbm, wu), (wd_hbm, wd)))
    ]
    for copy in weights:
        copy.start()

    def at(k):
        return lax.rem(z + k, zs)

    def device(k, dx, dy):
        return {
            "rep": (y + dy * (1 - 2 * y)) * 2 + core,
            "grp": at(k) * 2 + x + dx * (1 - 2 * x),
        }

    def block(k, da, db):
        dx = da * (1 - core) + db * core
        dy = db * (1 - core) + da * core
        return ((y + dy * (1 - 2 * y)) * zs + at(k)) * 2 + x + dx * (1 - 2 * x)

    a_dev = device(0, 1 - core, core)
    b_dev = device(0, core, 1 - core)
    x_dev = device(0, 1, 0)
    partner = {"rep": rep + 1 - 2 * core, "grp": grp}

    def copy_to(src, dst, s, r, dev):
        return pltpu.make_async_remote_copy(
            src_ref=src, dst_ref=dst, send_sem=s, recv_sem=r, device_id=dev, device_id_type=MESH
        )

    barrier = pltpu.get_barrier_semaphore()
    for dev in (partner, a_dev, b_dev):
        pl.semaphore_signal(barrier, inc=1, device_id=dev, device_id_type=MESH)

    def loop(low, high, body):
        def step(i, carry):
            body(i)
            return carry

        lax.fori_loop(low, high, step, 0)

    loop(
        1,
        zs,
        lambda k: pl.semaphore_signal(
            barrier, inc=1, device_id=device(k, 0, 0), device_id_type=MESH
        ),
    )
    pl.semaphore_wait(barrier, zs + 2)

    def to_x(k):
        return copy_to(
            part.at[at(k) * 2 + 1 - x], ra.at[at(k)], a_s.at[at(k)], a_r.at[at(k)], x_dev
        )

    loop(1, zs + 1, lambda k: to_x(k).start())

    def to_z(k):
        return copy_to(sz.at[k], rz.at[k], z_s.at[k], z_r.at[k], device(k, 0, 0))

    def sum_x(k):
        to_x(k).wait_recv()
        sz[k] = (part[at(k) * 2 + x].astype(f32) + ra[at(k)].astype(f32)).astype(sz.dtype)

        @pl.when(k > 1)
        def _():
            to_z(k - 1).start()

    loop(1, zs, sum_x)
    to_x(0).wait_recv()
    resid[...] = hid[...].astype(f32) + part[z * 2 + x].astype(f32) + ra[z].astype(f32)
    to_z(zs - 1).start()

    def sum_z(k):
        to_z(k).wait_recv()
        resid[...] += rz[k].astype(f32)

    loop(1, zs, sum_z)
    rounded = resid[...].astype(hid.dtype).astype(f32)
    resid[...] = rounded
    ssq = jnp.sum(rounded * rounded, axis=1, keepdims=True)
    ssq_out[...] = jnp.broadcast_to(ssq, ssq_out.shape)
    to_q = copy_to(ssq_out, ssq_in, q_s, q_r, partner)
    to_q.start()
    to_q.wait()
    mean_sq = (ssq + ssq_in[:, 0:1]) / (2 * half)
    mine = block(0, 0, 0)
    rows[mine, :, own_cols] = (
        resid[...] * lax.rsqrt(mean_sq + epsilon) * gain[...].astype(f32)
    ).astype(rows.dtype)

    def piece(k, da, db):
        return rows.at[block(zs - k, da, db), :, own_cols]

    def gather_z(k, source):
        return copy_to(
            piece(source, 0, 0), piece(source, 0, 0), gz_s.at[k], gz_r.at[k], device(k, 0, 0)
        )

    def gather_a(k, da):
        return copy_to(piece(k, da, 0), piece(k, da, 0), ga_s.at[k], ga_r.at[k], a_dev)

    def gather_b(k, da, db):
        j = da * zs + k
        return copy_to(piece(k, da, db), piece(k, da, db), gb_s.at[j], gb_r.at[j], b_dev)

    def relay(k, da, db, cols):
        j = k * 4 + da * (2 - core) + db * (1 + core)
        ref = rows.at[block(zs - k, da, db), :, cols]
        return copy_to(ref, ref, gp_s.at[j], gp_r.at[j], partner)

    loop(1, zs, lambda k: gather_z(k, 0).start())
    gather_b(0, 0, 0).start()
    gather_a(0, 0).start()
    relay(0, 0, 0, own_cols).start()

    def from_z(k):
        gather_z(k, k).wait_recv()
        gather_b(k, 0, 0).start()
        gather_a(k, 0).start()
        relay(k, 0, 0, own_cols).start()

    loop(1, zs, from_z)

    def from_a(k):
        gather_a(k, 1).wait_recv()
        gather_b(k, 1, 0).start()
        relay(k, 1, 0, own_cols).start()

    loop(0, zs, from_a)

    def from_b(j):
        da = lax.div(j, zs)
        k = lax.rem(j, zs)
        gather_b(k, da, 1).wait_recv()
        relay(k, da, 1, own_cols).start()

    loop(0, 2 * zs, from_b)

    def from_partner(j):
        da = lax.rem(lax.div(j, 2), 2)
        db = lax.rem(j, 2)
        relay(lax.div(j, 4), da, db, far_cols).wait_recv()

    loop(0, 4 * zs, from_partner)

    count = rows.shape[0] * rows.shape[1]
    depth = rows.shape[2] // 7
    weights[0].wait()
    weights[1].wait()
    acc_g[...] = jnp.zeros_like(acc_g)
    acc_u[...] = jnp.zeros_like(acc_u)

    def project(i):
        cols = pl.ds(pl.multiple_of(i * depth, 128), depth)
        lhs = rows[:, :, cols].reshape(count, depth)
        acc_g[...] += jnp.dot(lhs, wg[cols, :], preferred_element_type=f32)
        acc_u[...] += jnp.dot(lhs, wu[cols, :], preferred_element_type=f32)

    loop(0, 7, project)
    act[...] = (jax.nn.silu(acc_g[...]) * acc_u[...]).astype(act.dtype)
    weights[2].wait()

    def to_partner(i):
        return copy_to(pout.at[i], pin.at[i], t_s.at[i], t_r.at[i], partner)

    def down(first, i):
        cols = pl.ds(pl.multiple_of(first * half + i * tile, 128), tile)
        return jnp.dot(act[...], wd[:, cols], preferred_element_type=f32)

    def down_far(i):
        pout[i] = down(1 - core, i).astype(pout.dtype).reshape(pout.shape[1:])

        @pl.when(i > 0)
        def _():
            to_partner(i - 1).start()

    loop(0, 7, down_far)
    own[0] = down(core, 0).reshape(own.shape[1:])
    to_partner(6).start()

    def down_own(i):
        own[i] = down(core, i).reshape(own.shape[1:])
        to_partner(i - 1).wait_recv()
        own[i - 1] += pin[i - 1].astype(f32)

    loop(1, 7, down_own)
    to_partner(6).wait_recv()
    own[6] += pin[6].astype(f32)

    def value(k, da, db):
        target = block(k, da, db)
        return jnp.concatenate([own[i, target] for i in range(7)], axis=1)

    def to_b(j):
        return copy_to(sb.at[j], rb.at[j], b2_s.at[j], b2_r.at[j], b_dev)

    def slot(i):
        return (1 - lax.div(i, zs)) * zs + lax.rem(lax.rem(i, zs) + 1, zs)

    def sum_b(i):
        j = slot(i)
        sb[j] = value(lax.rem(j, zs), lax.div(j, zs), 1).astype(sb.dtype)

        @pl.when(i > 0)
        def _():
            to_b(slot(i - 1)).start()

    loop(0, 2 * zs, sum_b)
    to_b(0).start()

    def to_a(k):
        return copy_to(sa2.at[k], ra2.at[k], a2_s.at[k], a2_r.at[k], a_dev)

    def sum_a(i):
        k = lax.rem(i + 1, zs)
        to_b(zs + k).wait_recv()
        sa2[k] = (value(k, 1, 0) + rb[zs + k].astype(f32)).astype(sa2.dtype)

        @pl.when(i > 0)
        def _():
            to_a(i).start()

    loop(0, zs, sum_a)
    to_a(0).start()

    def to_z2(k):
        return copy_to(sz2.at[k], rz2.at[k], z2_s.at[k], z2_r.at[k], device(k, 0, 0))

    def so_far(k):
        to_b(k).wait_recv()
        to_a(k).wait_recv()
        return value(k, 0, 0) + rb[k].astype(f32) + ra2[k].astype(f32)

    def sum_z2(k):
        sz2[k] = so_far(k).astype(sz2.dtype)

        @pl.when(k > 1)
        def _():
            to_z2(k - 1).start()

    loop(1, zs, sum_z2)
    resid[...] += so_far(0)
    to_z2(zs - 1).start()

    def take_z2(k):
        to_z2(k).wait_recv()
        resid[...] += rz2[k].astype(f32)

    loop(1, zs, take_z2)
    out[:, own_cols] = resid[...].astype(out.dtype)

    def final(cols):
        return copy_to(out.at[:, cols], out.at[:, cols], f_s, f_r, partner)

    final(own_cols).start()

    loop(1, zs + 1, lambda k: to_x(k).wait_send())
    loop(0, 7, lambda i: to_partner(i).wait_send())

    def drain_z(k):
        to_z(k).wait_send()
        gather_z(k, 0).wait_send()
        to_z2(k).wait_send()

    loop(1, zs, drain_z)

    def drain_a(k):
        gather_a(k, 0).wait_send()
        to_a(k).wait_send()

    loop(0, zs, drain_a)

    def drain_b(j):
        gather_b(lax.rem(j, zs), lax.div(j, zs), 0).wait_send()
        to_b(j).wait_send()

    loop(0, 2 * zs, drain_b)

    def drain_relay(j):
        da = lax.rem(lax.div(j, 2), 2)
        relay(lax.div(j, 4), da, lax.rem(j, 2), own_cols).wait_send()

    loop(0, 4 * zs, drain_relay)
    final(far_cols).wait_recv()
    final(own_cols).wait_send()


def mlp_all(part, hid, gain, w_gate, w_up, w_down, group, cid):
    zs = group // 2
    eight, half = part.shape[1:]
    width = 2 * half
    hidden = w_gate.shape[1]
    count = 4 * zs * eight
    bf16, f32 = jnp.bfloat16, jnp.float32
    vmem = pl.BlockSpec(memory_space=pltpu.VMEM)
    hbm = pl.BlockSpec(memory_space=pltpu.HBM)

    def blocks(n):
        return pltpu.VMEM((n, eight, half), bf16)

    def sems(*counts):
        return [pltpu.SemaphoreType.DMA((n,)) for n in counts for _ in range(2)]

    one = [pltpu.SemaphoreType.DMA, pltpu.SemaphoreType.DMA]
    return pl.pallas_call(
        functools.partial(_mlp_kernel, zs),
        out_shape=jax.ShapeDtypeStruct((eight, width), bf16),
        in_specs=[vmem] * 3 + [hbm] * 3,
        out_specs=vmem,
        scratch_shapes=[
            pltpu.VMEM((width, hidden), bf16),
            pltpu.VMEM((width, hidden), bf16),
            pltpu.VMEM((hidden, width), bf16),
            blocks(zs),
            blocks(zs),
            blocks(zs),
            pltpu.VMEM((eight, 128), f32),
            pltpu.VMEM((eight, 128), f32),
            pltpu.VMEM((4 * zs, eight, width), bf16),
            pltpu.VMEM((count, hidden), f32),
            pltpu.VMEM((count, hidden), f32),
            pltpu.VMEM((count, hidden), bf16),
            pltpu.VMEM((7, 4 * zs, eight, half // 7), bf16),
            pltpu.VMEM((7, 4 * zs, eight, half // 7), bf16),
            pltpu.VMEM((7, 4 * zs, eight, half // 7), f32),
            blocks(2 * zs),
            blocks(2 * zs),
            blocks(zs),
            blocks(zs),
            blocks(zs),
            blocks(zs),
            pltpu.VMEM((eight, half), f32),
            pltpu.SemaphoreType.DMA((3,)),
        ]
        + sems(zs, zs)
        + one
        + sems(zs, zs, 2 * zs, 4 * zs, 7, 2 * zs, zs, zs)
        + one,
        compiler_params=pltpu.CompilerParams(
            collective_id=cid, has_side_effects=True, vmem_limit_bytes=60 * 1024 * 1024
        ),
    )(part, hid, gain, w_gate, w_up, w_down)


def on_device(
    rep_count,
    group,
    hidden_in,
    q_nope,
    q_rope,
    new_kv,
    cache_kv,
    lengths,
    w_uk,
    w_uv,
    w_out,
    norm_gain,
    w_gate,
    w_up,
    w_down,
):
    seq_count = hidden_in.shape[0]
    heads_here = H // group
    slice_width = w_uk.shape[0]
    grp = lax.axis_index("grp")
    rep = lax.axis_index("rep")

    q_rows = exchange(q_nope.reshape(seq_count * H, NOPE), "rep", rep_count, True, 1)
    q_part = jnp.einsum(
        "bhd,chd->bhc",
        q_rows.reshape(rep_count * seq_count, H, NOPE),
        w_uk.reshape(slice_width, H, NOPE),
        preferred_element_type=jnp.float32,
    ).astype(jnp.bfloat16)
    q_back = exchange(
        q_part.reshape(rep_count, seq_count * H, slice_width), "rep", rep_count, False, 2
    )
    uv_own = lax.dynamic_slice_in_dim(w_uv, grp * heads_here * VH, heads_here * VH, 1)
    uv_own, q_back = lax.optimization_barrier((uv_own, q_back))
    uv_parts = jnp.zeros((rep_count,) + uv_own.shape, uv_own.dtype)
    uv_parts = lax.dynamic_update_slice_in_dim(uv_parts, uv_own[None], rep, 0)
    for step in range(1, rep_count):
        moved = lax.ppermute(
            uv_own, "rep", [(i, (i + step) % rep_count) for i in range(rep_count)]
        )
        source = lax.rem(rep + rep_count - step, rep_count)
        uv_parts = lax.dynamic_update_slice_in_dim(uv_parts, moved[None], source, 0)
    value_up = uv_parts.reshape(KV_RANK, heads_here, VH)

    q_lat = q_back.reshape(rep_count, seq_count, H, slice_width)
    queries = jnp.concatenate(
        [q_lat[i] for i in range(rep_count)] + [q_rope.reshape(seq_count, H, ROPE)], axis=2
    )
    score_scale = float(NOPE + ROPE) ** (-0.5)
    scores = (
        jnp.einsum("bhc,blc->bhl", queries, cache_kv, preferred_element_type=jnp.float32)
        * score_scale
    )
    positions = lax.broadcasted_iota(jnp.int32, (1, 1, CACHE), 2)
    scores = jnp.where(positions < lengths[:, None, None], scores, -jnp.inf)
    own_score = (
        jnp.einsum("bhc,bc->bh", queries, new_kv, preferred_element_type=jnp.float32) * score_scale
    )
    row_top = jnp.maximum(jnp.max(scores, axis=2), own_score)
    weights = jnp.exp(scores - row_top[:, :, None])
    own_weight = jnp.exp(own_score - row_top)
    denom_sum = jnp.sum(weights, axis=2) + own_weight
    softmax_w = (weights / denom_sum[:, :, None]).astype(jnp.bfloat16)
    own_prob = (own_weight / denom_sum).astype(jnp.bfloat16)
    mixture = jnp.einsum("bhl,blc->bhc", softmax_w, cache_kv, preferred_element_type=jnp.float32)
    mixture = (
        mixture + own_prob.astype(jnp.float32)[:, :, None] * new_kv.astype(jnp.float32)[:, None, :]
    )
    latent = mixture[:, :, :KV_RANK].astype(jnp.bfloat16)

    by_heads = latent.reshape(seq_count, group, heads_here, KV_RANK).transpose(1, 0, 2, 3)
    latent_here = exchange(
        by_heads.reshape(group, seq_count * heads_here, KV_RANK), "grp", group, False, 3
    ).reshape(group * seq_count, heads_here, KV_RANK)
    head_out = jnp.einsum(
        "bhc,che->bhe", latent_here, value_up, preferred_element_type=jnp.float32
    ).astype(jnp.bfloat16)
    core = lax.rem(rep, 2)
    half = w_out.shape[1] // 2
    head_pair, hidden_pair = pair_gather(
        head_out.reshape(group * seq_count, heads_here * VH), hidden_in, 4
    )
    chip_rows = (
        head_pair.reshape(2, group, seq_count, -1)
        .transpose(1, 0, 2, 3)
        .reshape(group * 2 * seq_count, -1)
    )
    part = half_product(jnp.full((1,), core, jnp.int32), chip_rows, w_out)
    hid = lax.dynamic_slice_in_dim(hidden_pair.reshape(2 * seq_count, -1), core * half, half, 1)
    gain = lax.dynamic_slice_in_dim(norm_gain[None], core * half, half, 1)
    total = mlp_all(
        part.reshape(group, 2 * seq_count, half), hid, gain, w_gate, w_up, w_down, group, 5
    )
    return lax.dynamic_slice_in_dim(total, core * seq_count, seq_count, 0)


def solution(mesh):
    return jax.shard_map(
        functools.partial(on_device, mesh.shape["rep"], mesh.shape["grp"]),
        mesh=mesh,
        in_specs=(
            P(("rep", "grp"), None),
            P(("rep", "grp"), None),
            P(("rep", "grp"), None),
            P(("rep", "grp"), None),
            P(("rep", "grp"), None, None),
            P(("rep", "grp")),
            P("rep", None),
            P("rep", None),
            P("grp", None),
            P(),
            P(None, ("rep", "grp")),
            P(None, ("rep", "grp")),
            P(("rep", "grp"), None),
        ),
        out_specs=P(("rep", "grp"), None),
        check_vma=False,
    )
```

```python
import functools

import jax
import jax.numpy as jnp
from jax import lax
from jax.experimental import pallas as pl
from jax.experimental.pallas import tpu as pltpu
from jax.sharding import PartitionSpec as P

H = 64
NOPE = 128
ROPE = 64
VH = 128
KV_RANK = 512
CACHE = 4096
MESH = pl.DeviceIdType.MESH
ROWS = (((1,), (1,)), ((), ()))

epsilon = 1e-06


def _exchange_kernel(axis, n, gather, x_ref, out_ref, send_sem, recv_sem, own_sem):
    me = lax.axis_index(axis)
    barrier = pltpu.get_barrier_semaphore()

    def greet(k, carry):
        peer = lax.rem(me + k, n)
        pl.semaphore_signal(barrier, inc=1, device_id={axis: peer}, device_id_type=MESH)
        return carry

    lax.fori_loop(1, n, greet, 0)
    own = pltpu.make_async_copy(x_ref if gather else x_ref.at[me], out_ref.at[me], own_sem)
    own.start()
    pl.semaphore_wait(barrier, n - 1)

    def send(k, carry):
        peer = lax.rem(me + k, n)
        pltpu.make_async_remote_copy(
            src_ref=x_ref if gather else x_ref.at[peer],
            dst_ref=out_ref.at[me],
            send_sem=send_sem.at[k - 1],
            recv_sem=recv_sem.at[k - 1],
            device_id={axis: peer},
            device_id_type=MESH,
        ).start()
        return carry

    lax.fori_loop(1, n, send, 0)
    own.wait()

    def finish(k, carry):
        source = lax.rem(me + n - k, n)
        peer = lax.rem(me + k, n)
        pltpu.make_async_remote_copy(
            src_ref=x_ref if gather else x_ref.at[peer],
            dst_ref=out_ref.at[source],
            send_sem=send_sem.at[k - 1],
            recv_sem=recv_sem.at[k - 1],
            device_id={axis: peer},
            device_id_type=MESH,
        ).wait()
        return carry

    lax.fori_loop(1, n, finish, 0)


def exchange(x, axis, n, gather, cid):
    out_shape = ((n,) + x.shape) if gather else x.shape
    return pl.pallas_call(
        functools.partial(_exchange_kernel, axis, n, gather),
        out_shape=jax.ShapeDtypeStruct(out_shape, x.dtype),
        in_specs=[pl.BlockSpec(memory_space=pltpu.VMEM)],
        out_specs=pl.BlockSpec(memory_space=pltpu.VMEM),
        scratch_shapes=[
            pltpu.SemaphoreType.DMA((n - 1,)),
            pltpu.SemaphoreType.DMA((n - 1,)),
            pltpu.SemaphoreType.DMA,
        ],
        compiler_params=pltpu.CompilerParams(collective_id=cid, has_side_effects=True),
    )(x)


def _pair_kernel(h_ref, r_ref, h_out, r_out, send_sem, recv_sem, own_sem):
    rep = lax.axis_index("rep")
    core = lax.rem(rep, 2)
    partner = {"rep": rep + 1 - 2 * core}
    barrier = pltpu.get_barrier_semaphore()
    pl.semaphore_signal(barrier, inc=1, device_id=partner, device_id_type=MESH)
    own = [
        pltpu.make_async_copy(src, dst.at[core], own_sem.at[i])
        for i, (src, dst) in enumerate(((h_ref, h_out), (r_ref, r_out)))
    ]
    for copy in own:
        copy.start()
    pl.semaphore_wait(barrier, 1)

    def remote(i, src, dst, slot):
        return pltpu.make_async_remote_copy(
            src_ref=src,
            dst_ref=dst.at[slot],
            send_sem=send_sem.at[i],
            recv_sem=recv_sem.at[i],
            device_id=partner,
            device_id_type=MESH,
        )

    remote(0, h_ref, h_out, core).start()
    remote(1, r_ref, r_out, core).start()
    for copy in own:
        copy.wait()
    remote(0, h_ref, h_out, 1 - core).wait()
    remote(1, r_ref, r_out, 1 - core).wait()


def pair_gather(heads, resid, cid):
    vmem = pl.BlockSpec(memory_space=pltpu.VMEM)
    return pl.pallas_call(
        _pair_kernel,
        out_shape=[jax.ShapeDtypeStruct((2,) + v.shape, v.dtype) for v in (heads, resid)],
        in_specs=[vmem] * 2,
        out_specs=[vmem] * 2,
        scratch_shapes=[pltpu.SemaphoreType.DMA((2,))] * 3,
        compiler_params=pltpu.CompilerParams(collective_id=cid, has_side_effects=True),
    )(heads, resid)


def _half_product_kernel(core_ref, x_ref, w_ref, out_ref):
    out_ref[...] = jnp.dot(x_ref[...], w_ref[...], preferred_element_type=jnp.float32).astype(
        out_ref.dtype
    )


def half_product(core, x, w):
    rows, depth = x.shape
    half = w.shape[1] // 2
    tile = half // 7
    return pl.pallas_call(
        _half_product_kernel,
        out_shape=jax.ShapeDtypeStruct((rows, half), x.dtype),
        grid_spec=pltpu.PrefetchScalarGridSpec(
            num_scalar_prefetch=1,
            grid=(7,),
            in_specs=[
                pl.BlockSpec((rows, depth), lambda i, core: (0, 0)),
                pl.BlockSpec((depth, tile), lambda i, core: (0, core[0] * 7 + i)),
            ],
            out_specs=pl.BlockSpec((rows, tile), lambda i, core: (0, i)),
        ),
    )(core, x, w)


def _mlp_kernel(
    zs,
    part,
    hid,
    gain,
    wg_hbm,
    wu_hbm,
    wd_hbm,
    out,
    wg,
    wu,
    wd,
    ra,
    sz,
    rz,
    ssq_out,
    ssq_in,
    rows,
    acc_g,
    acc_u,
    act,
    pout,
    pin,
    own,
    sb,
    rb,
    sa2,
    ra2,
    sz2,
    rz2,
    resid,
    w_sem,
    a_s,
    a_r,
    z_s,
    z_r,
    q_s,
    q_r,
    gz_s,
    gz_r,
    ga_s,
    ga_r,
    gb_s,
    gb_r,
    gp_s,
    gp_r,
    t_s,
    t_r,
    b2_s,
    b2_r,
    a2_s,
    a2_r,
    z2_s,
    z2_r,
    f_s,
    f_r,
):
    rep = lax.axis_index("rep")
    grp = lax.axis_index("grp")
    core = lax.rem(rep, 2)
    y = lax.div(rep, 2)
    z = lax.div(grp, 2)
    x = lax.rem(grp, 2)
    half = part.shape[2]
    tile = half // 7
    own_cols = pl.ds(pl.multiple_of(core * half, 128), half)
    far_cols = pl.ds(pl.multiple_of((1 - core) * half, 128), half)
    f32 = jnp.float32

    weights = [
        pltpu.make_async_copy(src, dst, w_sem.at[i])
        for i, (src, dst) in enumerate(((wg_hbm, wg), (wu_hbm, wu), (wd_hbm, wd)))
    ]
    for copy in weights:
        copy.start()

    def at(k):
        return lax.rem(z + k, zs)

    def device(k, dx, dy):
        return {
            "rep": (y + dy * (1 - 2 * y)) * 2 + core,
            "grp": at(k) * 2 + x + dx * (1 - 2 * x),
        }

    def block(k, da, db):
        dx = da * (1 - core) + db * core
        dy = db * (1 - core) + da * core
        return ((y + dy * (1 - 2 * y)) * zs + at(k)) * 2 + x + dx * (1 - 2 * x)

    a_dev = device(0, 1 - core, core)
    b_dev = device(0, core, 1 - core)
    x_dev = device(0, 1, 0)
    partner = {"rep": rep + 1 - 2 * core, "grp": grp}

    def copy_to(src, dst, s, r, dev):
        return pltpu.make_async_remote_copy(
            src_ref=src, dst_ref=dst, send_sem=s, recv_sem=r, device_id=dev, device_id_type=MESH
        )

    barrier = pltpu.get_barrier_semaphore()
    for dev in (partner, a_dev, b_dev):
        pl.semaphore_signal(barrier, inc=1, device_id=dev, device_id_type=MESH)

    def loop(low, high, body):
        def step(i, carry):
            body(i)
            return carry

        lax.fori_loop(low, high, step, 0)

    loop(
        1,
        zs,
        lambda k: pl.semaphore_signal(
            barrier, inc=1, device_id=device(k, 0, 0), device_id_type=MESH
        ),
    )
    pl.semaphore_wait(barrier, zs + 2)

    def to_x(k):
        return copy_to(
            part.at[at(k) * 2 + 1 - x], ra.at[at(k)], a_s.at[at(k)], a_r.at[at(k)], x_dev
        )

    loop(1, zs + 1, lambda k: to_x(k).start())

    def to_z(k):
        return copy_to(sz.at[k], rz.at[k], z_s.at[k], z_r.at[k], device(k, 0, 0))

    def sum_x(k):
        to_x(k).wait_recv()
        sz[k] = (part[at(k) * 2 + x].astype(f32) + ra[at(k)].astype(f32)).astype(sz.dtype)

        @pl.when(k > 1)
        def _():
            to_z(k - 1).start()

    loop(1, zs, sum_x)
    to_x(0).wait_recv()
    resid[...] = hid[...].astype(f32) + part[z * 2 + x].astype(f32) + ra[z].astype(f32)
    to_z(zs - 1).start()

    def sum_z(k):
        to_z(k).wait_recv()
        resid[...] += rz[k].astype(f32)

    loop(1, zs, sum_z)
    rounded = resid[...].astype(hid.dtype).astype(f32)
    resid[...] = rounded
    ssq = jnp.sum(rounded * rounded, axis=1, keepdims=True)
    ssq_out[...] = jnp.broadcast_to(ssq, ssq_out.shape)
    to_q = copy_to(ssq_out, ssq_in, q_s, q_r, partner)
    to_q.start()
    to_q.wait()
    mean_sq = (ssq + ssq_in[:, 0:1]) / (2 * half)
    mine = block(0, 0, 0)
    rows[mine, :, own_cols] = (
        resid[...] * lax.rsqrt(mean_sq + epsilon) * gain[...].astype(f32)
    ).astype(rows.dtype)

    def piece(k, da, db):
        return rows.at[block(zs - k, da, db), :, own_cols]

    def gather_z(k, source):
        return copy_to(
            piece(source, 0, 0), piece(source, 0, 0), gz_s.at[k], gz_r.at[k], device(k, 0, 0)
        )

    def gather_a(k, da):
        return copy_to(piece(k, da, 0), piece(k, da, 0), ga_s.at[k], ga_r.at[k], a_dev)

    def gather_b(k, da, db):
        j = da * zs + k
        return copy_to(piece(k, da, db), piece(k, da, db), gb_s.at[j], gb_r.at[j], b_dev)

    def relay(k, da, db, cols):
        j = k * 4 + da * (2 - core) + db * (1 + core)
        ref = rows.at[block(zs - k, da, db), :, cols]
        return copy_to(ref, ref, gp_s.at[j], gp_r.at[j], partner)

    loop(1, zs, lambda k: gather_z(k, 0).start())
    gather_b(0, 0, 0).start()
    gather_a(0, 0).start()
    relay(0, 0, 0, own_cols).start()

    def from_z(k):
        gather_z(k, k).wait_recv()
        gather_b(k, 0, 0).start()
        gather_a(k, 0).start()
        relay(k, 0, 0, own_cols).start()

    loop(1, zs, from_z)

    def from_a(k):
        gather_a(k, 1).wait_recv()
        gather_b(k, 1, 0).start()
        relay(k, 1, 0, own_cols).start()

    loop(0, zs, from_a)

    def from_b(j):
        da = lax.div(j, zs)
        k = lax.rem(j, zs)
        gather_b(k, da, 1).wait_recv()
        relay(k, da, 1, own_cols).start()

    loop(0, 2 * zs, from_b)

    def from_partner(j):
        da = lax.rem(lax.div(j, 2), 2)
        db = lax.rem(j, 2)
        relay(lax.div(j, 4), da, db, far_cols).wait_recv()

    loop(0, 4 * zs, from_partner)

    count = rows.shape[0] * rows.shape[1]
    depth = rows.shape[2] // 7
    weights[0].wait()
    weights[1].wait()
    acc_g[...] = jnp.zeros_like(acc_g)
    acc_u[...] = jnp.zeros_like(acc_u)

    def project(i):
        cols = pl.ds(pl.multiple_of(i * depth, 128), depth)
        lhs = rows[:, :, cols].reshape(count, depth)
        acc_g[...] += lax.dot_general(lhs, wg[:, cols], ROWS, preferred_element_type=f32)
        acc_u[...] += lax.dot_general(lhs, wu[:, cols], ROWS, preferred_element_type=f32)

    loop(0, 7, project)
    act[...] = (jax.nn.silu(acc_g[...]) * acc_u[...]).astype(act.dtype)
    weights[2].wait()

    def to_partner(i):
        return copy_to(pout.at[i], pin.at[i], t_s.at[i], t_r.at[i], partner)

    def down(first, i):
        cols = pl.ds(pl.multiple_of(first * half + i * tile, 128), tile)
        return jnp.dot(act[...], wd[:, cols], preferred_element_type=f32)

    def down_far(i):
        pout[i] = down(1 - core, i).astype(pout.dtype).reshape(pout.shape[1:])

        @pl.when(i > 0)
        def _():
            to_partner(i - 1).start()

    loop(0, 7, down_far)
    own[0] = down(core, 0).reshape(own.shape[1:])
    to_partner(6).start()

    def down_own(i):
        own[i] = down(core, i).reshape(own.shape[1:])
        to_partner(i - 1).wait_recv()
        own[i - 1] += pin[i - 1].astype(f32)

    loop(1, 7, down_own)
    to_partner(6).wait_recv()
    own[6] += pin[6].astype(f32)

    def value(k, da, db):
        target = block(k, da, db)
        return jnp.concatenate([own[i, target] for i in range(7)], axis=1)

    def to_b(j):
        return copy_to(sb.at[j], rb.at[j], b2_s.at[j], b2_r.at[j], b_dev)

    def slot(i):
        return (1 - lax.div(i, zs)) * zs + lax.rem(lax.rem(i, zs) + 1, zs)

    def sum_b(i):
        j = slot(i)
        sb[j] = value(lax.rem(j, zs), lax.div(j, zs), 1).astype(sb.dtype)

        @pl.when(i > 0)
        def _():
            to_b(slot(i - 1)).start()

    loop(0, 2 * zs, sum_b)
    to_b(0).start()

    def to_a(k):
        return copy_to(sa2.at[k], ra2.at[k], a2_s.at[k], a2_r.at[k], a_dev)

    def sum_a(i):
        k = lax.rem(i + 1, zs)
        to_b(zs + k).wait_recv()
        sa2[k] = (value(k, 1, 0) + rb[zs + k].astype(f32)).astype(sa2.dtype)

        @pl.when(i > 0)
        def _():
            to_a(i).start()

    loop(0, zs, sum_a)
    to_a(0).start()

    def to_z2(k):
        return copy_to(sz2.at[k], rz2.at[k], z2_s.at[k], z2_r.at[k], device(k, 0, 0))

    def so_far(k):
        to_b(k).wait_recv()
        to_a(k).wait_recv()
        return value(k, 0, 0) + rb[k].astype(f32) + ra2[k].astype(f32)

    def sum_z2(k):
        sz2[k] = so_far(k).astype(sz2.dtype)

        @pl.when(k > 1)
        def _():
            to_z2(k - 1).start()

    loop(1, zs, sum_z2)
    resid[...] += so_far(0)
    to_z2(zs - 1).start()

    def take_z2(k):
        to_z2(k).wait_recv()
        resid[...] += rz2[k].astype(f32)

    loop(1, zs, take_z2)
    out[:, own_cols] = resid[...].astype(out.dtype)

    def final(cols):
        return copy_to(out.at[:, cols], out.at[:, cols], f_s, f_r, partner)

    final(own_cols).start()

    loop(1, zs + 1, lambda k: to_x(k).wait_send())
    loop(0, 7, lambda i: to_partner(i).wait_send())

    def drain_z(k):
        to_z(k).wait_send()
        gather_z(k, 0).wait_send()
        to_z2(k).wait_send()

    loop(1, zs, drain_z)

    def drain_a(k):
        gather_a(k, 0).wait_send()
        to_a(k).wait_send()

    loop(0, zs, drain_a)

    def drain_b(j):
        gather_b(lax.rem(j, zs), lax.div(j, zs), 0).wait_send()
        to_b(j).wait_send()

    loop(0, 2 * zs, drain_b)

    def drain_relay(j):
        da = lax.rem(lax.div(j, 2), 2)
        relay(lax.div(j, 4), da, lax.rem(j, 2), own_cols).wait_send()

    loop(0, 4 * zs, drain_relay)
    final(far_cols).wait_recv()
    final(own_cols).wait_send()


def mlp_all(part, hid, gain, w_gate, w_up, w_down, group, cid):
    zs = group // 2
    eight, half = part.shape[1:]
    width = 2 * half
    hidden = w_gate.shape[0]
    count = 4 * zs * eight
    bf16, f32 = jnp.bfloat16, jnp.float32
    vmem = pl.BlockSpec(memory_space=pltpu.VMEM)
    hbm = pl.BlockSpec(memory_space=pltpu.HBM)

    def blocks(n):
        return pltpu.VMEM((n, eight, half), bf16)

    def sems(*counts):
        return [pltpu.SemaphoreType.DMA((n,)) for n in counts for _ in range(2)]

    one = [pltpu.SemaphoreType.DMA, pltpu.SemaphoreType.DMA]
    return pl.pallas_call(
        functools.partial(_mlp_kernel, zs),
        out_shape=jax.ShapeDtypeStruct((eight, width), bf16),
        in_specs=[vmem] * 3 + [hbm] * 3,
        out_specs=vmem,
        scratch_shapes=[
            pltpu.VMEM((hidden, width), bf16),
            pltpu.VMEM((hidden, width), bf16),
            pltpu.VMEM((hidden, width), bf16),
            blocks(zs),
            blocks(zs),
            blocks(zs),
            pltpu.VMEM((eight, 128), f32),
            pltpu.VMEM((eight, 128), f32),
            pltpu.VMEM((4 * zs, eight, width), bf16),
            pltpu.VMEM((count, hidden), f32),
            pltpu.VMEM((count, hidden), f32),
            pltpu.VMEM((count, hidden), bf16),
            pltpu.VMEM((7, 4 * zs, eight, half // 7), bf16),
            pltpu.VMEM((7, 4 * zs, eight, half // 7), bf16),
            pltpu.VMEM((7, 4 * zs, eight, half // 7), f32),
            blocks(2 * zs),
            blocks(2 * zs),
            blocks(zs),
            blocks(zs),
            blocks(zs),
            blocks(zs),
            pltpu.VMEM((eight, half), f32),
            pltpu.SemaphoreType.DMA((3,)),
        ]
        + sems(zs, zs)
        + one
        + sems(zs, zs, 2 * zs, 4 * zs, 7, 2 * zs, zs, zs)
        + one,
        compiler_params=pltpu.CompilerParams(
            collective_id=cid, has_side_effects=True, vmem_limit_bytes=60 * 1024 * 1024
        ),
    )(part, hid, gain, w_gate, w_up, w_down)


def _attend_kernel(tile, lengths, q_ref, new_ref, cache_ref, out_ref, top, denom, acc):
    b = pl.program_id(0)
    j = pl.program_id(1)
    f32 = jnp.float32
    scale = float(NOPE + ROPE) ** (-0.5)

    @pl.when(j == 0)
    def _():
        own = q_ref[0].astype(f32) * new_ref[0].astype(f32)
        top[...] = jnp.sum(own, axis=1, keepdims=True) * scale
        denom[...] = jnp.ones_like(denom)
        acc[...] = jnp.broadcast_to(new_ref[0][:, :KV_RANK].astype(f32), acc.shape)

    @pl.when(j * tile < lengths[b])
    def _():
        cache = cache_ref[0]
        scores = jnp.dot(q_ref[0], cache, preferred_element_type=f32) * scale
        positions = j * tile + lax.broadcasted_iota(jnp.int32, (1, tile), 1)
        scores = jnp.where(positions < lengths[b], scores, -jnp.inf)
        new_top = jnp.maximum(top[...], jnp.max(scores, axis=1, keepdims=True))
        weights = jnp.exp(scores - new_top)
        shrink = jnp.exp(top[...] - new_top)
        denom[...] = shrink * denom[...] + jnp.sum(weights, axis=1, keepdims=True)
        acc[...] = shrink * acc[...] + lax.dot_general(
            weights.astype(cache.dtype), cache[:KV_RANK], ROWS, preferred_element_type=f32
        )
        top[...] = new_top

    @pl.when(j == pl.num_programs(1) - 1)
    def _():
        out_ref[0] = (acc[...] / denom[...]).astype(out_ref.dtype)


def attend(lengths, queries, new_kv, cache_kv):
    seq_count, length, width = cache_kv.shape
    tile = length // 4
    return pl.pallas_call(
        functools.partial(_attend_kernel, tile),
        out_shape=jax.ShapeDtypeStruct((seq_count, H, KV_RANK), queries.dtype),
        grid_spec=pltpu.PrefetchScalarGridSpec(
            num_scalar_prefetch=1,
            grid=(seq_count, 4),
            in_specs=[
                pl.BlockSpec((1, H, width), lambda b, j, n: (b, 0, 0)),
                pl.BlockSpec((1, 1, width), lambda b, j, n: (b, 0, 0)),
                pl.BlockSpec(
                    (1, width, tile),
                    lambda b, j, n: (b, 0, jnp.minimum(j, lax.div(n[b] - 1, tile))),
                ),
            ],
            out_specs=pl.BlockSpec((1, H, KV_RANK), lambda b, j, n: (b, 0, 0)),
            scratch_shapes=[
                pltpu.VMEM((H, 1), jnp.float32),
                pltpu.VMEM((H, 1), jnp.float32),
                pltpu.VMEM((H, KV_RANK), jnp.float32),
            ],
        ),
        cost_estimate=pl.CostEstimate(
            flops=4 * seq_count * H * length * width,
            bytes_accessed=2 * cache_kv.size,
            transcendentals=seq_count * H * length,
        ),
    )(lengths, queries, new_kv.reshape(seq_count, 1, width), jnp.swapaxes(cache_kv, 1, 2))


def on_device(
    rep_count,
    group,
    hidden_in,
    q_nope,
    q_rope,
    new_kv,
    cache_kv,
    lengths,
    w_uk,
    w_uv,
    w_out,
    norm_gain,
    w_gate,
    w_up,
    w_down,
):
    seq_count = hidden_in.shape[0]
    heads_here = H // group
    slice_width = w_uk.shape[0]
    grp = lax.axis_index("grp")
    rep = lax.axis_index("rep")

    q_rows = exchange(q_nope.reshape(seq_count * H, NOPE), "rep", rep_count, True, 1)
    q_part = jnp.einsum(
        "bhd,chd->bhc",
        q_rows.reshape(rep_count * seq_count, H, NOPE),
        w_uk.reshape(slice_width, H, NOPE),
        preferred_element_type=jnp.float32,
    ).astype(jnp.bfloat16)
    q_back = exchange(
        q_part.reshape(rep_count, seq_count * H, slice_width), "rep", rep_count, False, 2
    )
    uv_own = lax.dynamic_slice_in_dim(w_uv, grp * heads_here * VH, heads_here * VH, 1)
    uv_own, q_back = lax.optimization_barrier((uv_own, q_back))
    uv_parts = jnp.zeros((rep_count,) + uv_own.shape, uv_own.dtype)
    uv_parts = lax.dynamic_update_slice_in_dim(uv_parts, uv_own[None], rep, 0)
    for step in range(1, rep_count):
        moved = lax.ppermute(
            uv_own, "rep", [(i, (i + step) % rep_count) for i in range(rep_count)]
        )
        source = lax.rem(rep + rep_count - step, rep_count)
        uv_parts = lax.dynamic_update_slice_in_dim(uv_parts, moved[None], source, 0)
    value_up = uv_parts.reshape(KV_RANK, heads_here, VH)

    q_lat = q_back.reshape(rep_count, seq_count, H, slice_width)
    queries = jnp.concatenate(
        [q_lat[i] for i in range(rep_count)] + [q_rope.reshape(seq_count, H, ROPE)], axis=2
    )
    latent = attend(lengths, queries, new_kv, cache_kv)

    by_heads = latent.reshape(seq_count, group, heads_here, KV_RANK).transpose(1, 0, 2, 3)
    latent_here = exchange(
        by_heads.reshape(group, seq_count * heads_here, KV_RANK), "grp", group, False, 3
    ).reshape(group * seq_count, heads_here, KV_RANK)
    head_out = jnp.einsum(
        "bhc,che->bhe", latent_here, value_up, preferred_element_type=jnp.float32
    ).astype(jnp.bfloat16)
    core = lax.rem(rep, 2)
    half = w_out.shape[1] // 2
    head_pair, hidden_pair = pair_gather(
        head_out.reshape(group * seq_count, heads_here * VH), hidden_in, 4
    )
    chip_rows = (
        head_pair.reshape(2, group, seq_count, -1)
        .transpose(1, 0, 2, 3)
        .reshape(group * 2 * seq_count, -1)
    )
    part = half_product(jnp.full((1,), core, jnp.int32), chip_rows, w_out)
    hid = lax.dynamic_slice_in_dim(hidden_pair.reshape(2 * seq_count, -1), core * half, half, 1)
    gain = lax.dynamic_slice_in_dim(norm_gain[None], core * half, half, 1)
    total = mlp_all(
        part.reshape(group, 2 * seq_count, half), hid, gain, w_gate.T, w_up.T, w_down, group, 5
    )
    return lax.dynamic_slice_in_dim(total, core * seq_count, seq_count, 0)


def solution(mesh):
    return jax.shard_map(
        functools.partial(on_device, mesh.shape["rep"], mesh.shape["grp"]),
        mesh=mesh,
        in_specs=(
            P(("rep", "grp"), None),
            P(("rep", "grp"), None),
            P(("rep", "grp"), None),
            P(("rep", "grp"), None),
            P(("rep", "grp"), None, None),
            P(("rep", "grp")),
            P("rep", None),
            P("rep", None),
            P("grp", None),
            P(),
            P(None, ("rep", "grp")),
            P(None, ("rep", "grp")),
            P(("rep", "grp"), None),
        ),
        out_specs=P(("rep", "grp"), None),
        check_vma=False,
    )
```

```python
import functools

import jax
import jax.numpy as jnp
from jax import lax
from jax.experimental import pallas as pl
from jax.experimental.pallas import tpu as pltpu
from jax.sharding import PartitionSpec as P

H = 64
NOPE = 128
ROPE = 64
VH = 128
KV_RANK = 512
CACHE = 4096
MESH = pl.DeviceIdType.MESH
ROWS = (((1,), (1,)), ((), ()))

epsilon = 1e-06


def _exchange_kernel(axis, n, gather, x_ref, out_ref, send_sem, recv_sem, own_sem):
    me = lax.axis_index(axis)
    barrier = pltpu.get_barrier_semaphore()

    def greet(k, carry):
        peer = lax.rem(me + k, n)
        pl.semaphore_signal(barrier, inc=1, device_id={axis: peer}, device_id_type=MESH)
        return carry

    lax.fori_loop(1, n, greet, 0)
    own = pltpu.make_async_copy(x_ref if gather else x_ref.at[me], out_ref.at[me], own_sem)
    own.start()
    pl.semaphore_wait(barrier, n - 1)

    def send(k, carry):
        peer = lax.rem(me + k, n)
        pltpu.make_async_remote_copy(
            src_ref=x_ref if gather else x_ref.at[peer],
            dst_ref=out_ref.at[me],
            send_sem=send_sem.at[k - 1],
            recv_sem=recv_sem.at[k - 1],
            device_id={axis: peer},
            device_id_type=MESH,
        ).start()
        return carry

    lax.fori_loop(1, n, send, 0)
    own.wait()

    def finish(k, carry):
        source = lax.rem(me + n - k, n)
        peer = lax.rem(me + k, n)
        pltpu.make_async_remote_copy(
            src_ref=x_ref if gather else x_ref.at[peer],
            dst_ref=out_ref.at[source],
            send_sem=send_sem.at[k - 1],
            recv_sem=recv_sem.at[k - 1],
            device_id={axis: peer},
            device_id_type=MESH,
        ).wait()
        return carry

    lax.fori_loop(1, n, finish, 0)


def exchange(x, axis, n, gather, cid):
    out_shape = ((n,) + x.shape) if gather else x.shape
    return pl.pallas_call(
        functools.partial(_exchange_kernel, axis, n, gather),
        out_shape=jax.ShapeDtypeStruct(out_shape, x.dtype),
        in_specs=[pl.BlockSpec(memory_space=pltpu.VMEM)],
        out_specs=pl.BlockSpec(memory_space=pltpu.VMEM),
        scratch_shapes=[
            pltpu.SemaphoreType.DMA((n - 1,)),
            pltpu.SemaphoreType.DMA((n - 1,)),
            pltpu.SemaphoreType.DMA,
        ],
        compiler_params=pltpu.CompilerParams(collective_id=cid, has_side_effects=True),
    )(x)


def _pair_kernel(h_ref, r_ref, h_out, r_out, send_sem, recv_sem, own_sem):
    rep = lax.axis_index("rep")
    core = lax.rem(rep, 2)
    partner = {"rep": rep + 1 - 2 * core}
    barrier = pltpu.get_barrier_semaphore()
    pl.semaphore_signal(barrier, inc=1, device_id=partner, device_id_type=MESH)
    own = [
        pltpu.make_async_copy(src, dst.at[core], own_sem.at[i])
        for i, (src, dst) in enumerate(((h_ref, h_out), (r_ref, r_out)))
    ]
    for copy in own:
        copy.start()
    pl.semaphore_wait(barrier, 1)

    def remote(i, src, dst, slot):
        return pltpu.make_async_remote_copy(
            src_ref=src,
            dst_ref=dst.at[slot],
            send_sem=send_sem.at[i],
            recv_sem=recv_sem.at[i],
            device_id=partner,
            device_id_type=MESH,
        )

    remote(0, h_ref, h_out, core).start()
    remote(1, r_ref, r_out, core).start()
    for copy in own:
        copy.wait()
    remote(0, h_ref, h_out, 1 - core).wait()
    remote(1, r_ref, r_out, 1 - core).wait()


def pair_gather(heads, resid, cid):
    vmem = pl.BlockSpec(memory_space=pltpu.VMEM)
    return pl.pallas_call(
        _pair_kernel,
        out_shape=[jax.ShapeDtypeStruct((2,) + v.shape, v.dtype) for v in (heads, resid)],
        in_specs=[vmem] * 2,
        out_specs=[vmem] * 2,
        scratch_shapes=[pltpu.SemaphoreType.DMA((2,))] * 3,
        compiler_params=pltpu.CompilerParams(collective_id=cid, has_side_effects=True),
    )(heads, resid)


def _half_product_kernel(core_ref, x_ref, w_ref, out_ref):
    out_ref[...] = jnp.dot(x_ref[...], w_ref[...], preferred_element_type=jnp.float32).astype(
        out_ref.dtype
    )


def half_product(core, x, w):
    rows, depth = x.shape
    half = w.shape[1] // 2
    tile = half // 7
    return pl.pallas_call(
        _half_product_kernel,
        out_shape=jax.ShapeDtypeStruct((rows, half), x.dtype),
        grid_spec=pltpu.PrefetchScalarGridSpec(
            num_scalar_prefetch=1,
            grid=(7,),
            in_specs=[
                pl.BlockSpec((rows, depth), lambda i, core: (0, 0)),
                pl.BlockSpec((depth, tile), lambda i, core: (0, core[0] * 7 + i)),
            ],
            out_specs=pl.BlockSpec((rows, tile), lambda i, core: (0, i)),
        ),
    )(core, x, w)


def _mlp_kernel(
    zs,
    part,
    hid,
    gain,
    wg_hbm,
    wu_hbm,
    wd_hbm,
    out,
    wg,
    wu,
    wd,
    ra,
    sz,
    rz,
    ssq_out,
    ssq_in,
    rows,
    acc_g,
    acc_u,
    act,
    pout,
    pin,
    own,
    sb,
    rb,
    sa2,
    ra2,
    sz2,
    rz2,
    resid,
    w_sem,
    a_s,
    a_r,
    z_s,
    z_r,
    q_s,
    q_r,
    gz_s,
    gz_r,
    ga_s,
    ga_r,
    gb_s,
    gb_r,
    gp_s,
    gp_r,
    t_s,
    t_r,
    b2_s,
    b2_r,
    a2_s,
    a2_r,
    z2_s,
    z2_r,
    f_s,
    f_r,
):
    rep = lax.axis_index("rep")
    grp = lax.axis_index("grp")
    core = lax.rem(rep, 2)
    y = lax.div(rep, 2)
    z = lax.div(grp, 2)
    x = lax.rem(grp, 2)
    half = part.shape[2]
    tile = half // 7
    own_cols = pl.ds(pl.multiple_of(core * half, 128), half)
    far_cols = pl.ds(pl.multiple_of((1 - core) * half, 128), half)
    f32 = jnp.float32

    weights = [
        pltpu.make_async_copy(src, dst, w_sem.at[i])
        for i, (src, dst) in enumerate(((wg_hbm, wg), (wu_hbm, wu), (wd_hbm, wd)))
    ]
    for copy in weights:
        copy.start()

    def at(k):
        return lax.rem(z + k, zs)

    def device(k, dx, dy):
        return {
            "rep": (y + dy * (1 - 2 * y)) * 2 + core,
            "grp": at(k) * 2 + x + dx * (1 - 2 * x),
        }

    def block(k, da, db):
        dx = da * (1 - core) + db * core
        dy = db * (1 - core) + da * core
        return ((y + dy * (1 - 2 * y)) * zs + at(k)) * 2 + x + dx * (1 - 2 * x)

    a_dev = device(0, 1 - core, core)
    b_dev = device(0, core, 1 - core)
    x_dev = device(0, 1, 0)
    partner = {"rep": rep + 1 - 2 * core, "grp": grp}

    def copy_to(src, dst, s, r, dev):
        return pltpu.make_async_remote_copy(
            src_ref=src, dst_ref=dst, send_sem=s, recv_sem=r, device_id=dev, device_id_type=MESH
        )

    barrier = pltpu.get_barrier_semaphore()
    for dev in (partner, a_dev, b_dev):
        pl.semaphore_signal(barrier, inc=1, device_id=dev, device_id_type=MESH)

    def loop(low, high, body):
        def step(i, carry):
            body(i)
            return carry

        lax.fori_loop(low, high, step, 0)

    loop(
        1,
        zs,
        lambda k: pl.semaphore_signal(
            barrier, inc=1, device_id=device(k, 0, 0), device_id_type=MESH
        ),
    )
    pl.semaphore_wait(barrier, zs + 2)

    def to_x(k):
        return copy_to(
            part.at[at(k) * 2 + 1 - x], ra.at[at(k)], a_s.at[at(k)], a_r.at[at(k)], x_dev
        )

    loop(1, zs + 1, lambda k: to_x(k).start())

    def to_z(k):
        return copy_to(sz.at[k], rz.at[k], z_s.at[k], z_r.at[k], device(k, 0, 0))

    def sum_x(k):
        to_x(k).wait_recv()
        sz[k] = (part[at(k) * 2 + x].astype(f32) + ra[at(k)].astype(f32)).astype(sz.dtype)

        @pl.when(k > 1)
        def _():
            to_z(k - 1).start()

    loop(1, zs, sum_x)
    to_x(0).wait_recv()
    resid[...] = hid[...].astype(f32) + part[z * 2 + x].astype(f32) + ra[z].astype(f32)
    to_z(zs - 1).start()

    def sum_z(k):
        to_z(k).wait_recv()
        resid[...] += rz[k].astype(f32)

    loop(1, zs, sum_z)
    rounded = resid[...].astype(hid.dtype).astype(f32)
    resid[...] = rounded
    ssq = jnp.sum(rounded * rounded, axis=1, keepdims=True)
    ssq_out[...] = jnp.broadcast_to(ssq, ssq_out.shape)
    to_q = copy_to(ssq_out, ssq_in, q_s, q_r, partner)
    to_q.start()
    to_q.wait()
    mean_sq = (ssq + ssq_in[:, 0:1]) / (2 * half)
    mine = block(0, 0, 0)
    rows[mine, :, own_cols] = (
        resid[...] * lax.rsqrt(mean_sq + epsilon) * gain[...].astype(f32)
    ).astype(rows.dtype)

    def piece(k, da, db):
        return rows.at[block(zs - k, da, db), :, own_cols]

    def gather_z(k, source):
        return copy_to(
            piece(source, 0, 0), piece(source, 0, 0), gz_s.at[k], gz_r.at[k], device(k, 0, 0)
        )

    def gather_a(k, da):
        return copy_to(piece(k, da, 0), piece(k, da, 0), ga_s.at[k], ga_r.at[k], a_dev)

    def gather_b(k, da, db):
        j = da * zs + k
        return copy_to(piece(k, da, db), piece(k, da, db), gb_s.at[j], gb_r.at[j], b_dev)

    def relay(k, da, db, cols):
        j = k * 4 + da * (2 - core) + db * (1 + core)
        ref = rows.at[block(zs - k, da, db), :, cols]
        return copy_to(ref, ref, gp_s.at[j], gp_r.at[j], partner)

    loop(1, zs, lambda k: gather_z(k, 0).start())
    gather_b(0, 0, 0).start()
    gather_a(0, 0).start()
    relay(0, 0, 0, own_cols).start()

    def from_z(k):
        gather_z(k, k).wait_recv()
        gather_b(k, 0, 0).start()
        gather_a(k, 0).start()
        relay(k, 0, 0, own_cols).start()

    loop(1, zs, from_z)

    def from_a(k):
        gather_a(k, 1).wait_recv()
        gather_b(k, 1, 0).start()
        relay(k, 1, 0, own_cols).start()

    loop(0, zs, from_a)

    def from_b(j):
        da = lax.div(j, zs)
        k = lax.rem(j, zs)
        gather_b(k, da, 1).wait_recv()
        relay(k, da, 1, own_cols).start()

    loop(0, 2 * zs, from_b)

    def from_partner(j):
        da = lax.rem(lax.div(j, 2), 2)
        db = lax.rem(j, 2)
        relay(lax.div(j, 4), da, db, far_cols).wait_recv()

    loop(0, 4 * zs, from_partner)

    count = rows.shape[0] * rows.shape[1]
    depth = rows.shape[2] // 7
    weights[0].wait()
    weights[1].wait()
    acc_g[...] = jnp.zeros_like(acc_g)
    acc_u[...] = jnp.zeros_like(acc_u)

    def project(i):
        cols = pl.ds(pl.multiple_of(i * depth, 128), depth)
        lhs = rows[:, :, cols].reshape(count, depth)
        acc_g[...] += lax.dot_general(lhs, wg[:, cols], ROWS, preferred_element_type=f32)
        acc_u[...] += lax.dot_general(lhs, wu[:, cols], ROWS, preferred_element_type=f32)

    loop(0, 7, project)
    act[...] = (jax.nn.silu(acc_g[...]) * acc_u[...]).astype(act.dtype)
    weights[2].wait()

    def to_partner(i):
        return copy_to(pout.at[i], pin.at[i], t_s.at[i], t_r.at[i], partner)

    def down(first, i):
        cols = pl.ds(pl.multiple_of(first * half + i * tile, 128), tile)
        return jnp.dot(act[...], wd[:, cols], preferred_element_type=f32)

    def down_far(i):
        pout[i] = down(1 - core, i).astype(pout.dtype).reshape(pout.shape[1:])

        @pl.when(i > 0)
        def _():
            to_partner(i - 1).start()

    loop(0, 7, down_far)
    own[0] = down(core, 0).reshape(own.shape[1:])
    to_partner(6).start()

    def down_own(i):
        own[i] = down(core, i).reshape(own.shape[1:])
        to_partner(i - 1).wait_recv()
        own[i - 1] += pin[i - 1].astype(f32)

    loop(1, 7, down_own)
    to_partner(6).wait_recv()
    own[6] += pin[6].astype(f32)

    def value(k, da, db):
        target = block(k, da, db)
        return jnp.concatenate([own[i, target] for i in range(7)], axis=1)

    def to_b(j):
        return copy_to(sb.at[j], rb.at[j], b2_s.at[j], b2_r.at[j], b_dev)

    def slot(i):
        return (1 - lax.div(i, zs)) * zs + lax.rem(lax.rem(i, zs) + 1, zs)

    def sum_b(i):
        j = slot(i)
        sb[j] = value(lax.rem(j, zs), lax.div(j, zs), 1).astype(sb.dtype)

        @pl.when(i > 0)
        def _():
            to_b(slot(i - 1)).start()

    loop(0, 2 * zs, sum_b)
    to_b(0).start()

    def to_a(k):
        return copy_to(sa2.at[k], ra2.at[k], a2_s.at[k], a2_r.at[k], a_dev)

    def sum_a(i):
        k = lax.rem(i + 1, zs)
        to_b(zs + k).wait_recv()
        sa2[k] = (value(k, 1, 0) + rb[zs + k].astype(f32)).astype(sa2.dtype)

        @pl.when(i > 0)
        def _():
            to_a(i).start()

    loop(0, zs, sum_a)
    to_a(0).start()

    def to_z2(k):
        return copy_to(sz2.at[k], rz2.at[k], z2_s.at[k], z2_r.at[k], device(k, 0, 0))

    def so_far(k):
        to_b(k).wait_recv()
        to_a(k).wait_recv()
        return value(k, 0, 0) + rb[k].astype(f32) + ra2[k].astype(f32)

    def sum_z2(k):
        sz2[k] = so_far(k).astype(sz2.dtype)

        @pl.when(k > 1)
        def _():
            to_z2(k - 1).start()

    loop(1, zs, sum_z2)
    resid[...] += so_far(0)
    to_z2(zs - 1).start()

    def take_z2(k):
        to_z2(k).wait_recv()
        resid[...] += rz2[k].astype(f32)

    loop(1, zs, take_z2)
    out[:, own_cols] = resid[...].astype(out.dtype)

    def final(cols):
        return copy_to(out.at[:, cols], out.at[:, cols], f_s, f_r, partner)

    final(own_cols).start()

    loop(1, zs + 1, lambda k: to_x(k).wait_send())
    loop(0, 7, lambda i: to_partner(i).wait_send())

    def drain_z(k):
        to_z(k).wait_send()
        gather_z(k, 0).wait_send()
        to_z2(k).wait_send()

    loop(1, zs, drain_z)

    def drain_a(k):
        gather_a(k, 0).wait_send()
        to_a(k).wait_send()

    loop(0, zs, drain_a)

    def drain_b(j):
        gather_b(lax.rem(j, zs), lax.div(j, zs), 0).wait_send()
        to_b(j).wait_send()

    loop(0, 2 * zs, drain_b)

    def drain_relay(j):
        da = lax.rem(lax.div(j, 2), 2)
        relay(lax.div(j, 4), da, lax.rem(j, 2), own_cols).wait_send()

    loop(0, 4 * zs, drain_relay)
    final(far_cols).wait_recv()
    final(own_cols).wait_send()


def mlp_all(part, hid, gain, w_gate, w_up, w_down, group, cid):
    zs = group // 2
    eight, half = part.shape[1:]
    width = 2 * half
    hidden = w_gate.shape[0]
    count = 4 * zs * eight
    bf16, f32 = jnp.bfloat16, jnp.float32
    vmem = pl.BlockSpec(memory_space=pltpu.VMEM)
    hbm = pl.BlockSpec(memory_space=pltpu.HBM)

    def blocks(n):
        return pltpu.VMEM((n, eight, half), bf16)

    def sems(*counts):
        return [pltpu.SemaphoreType.DMA((n,)) for n in counts for _ in range(2)]

    one = [pltpu.SemaphoreType.DMA, pltpu.SemaphoreType.DMA]
    return pl.pallas_call(
        functools.partial(_mlp_kernel, zs),
        out_shape=jax.ShapeDtypeStruct((eight, width), bf16),
        in_specs=[vmem] * 3 + [hbm] * 3,
        out_specs=vmem,
        scratch_shapes=[
            pltpu.VMEM((hidden, width), bf16),
            pltpu.VMEM((hidden, width), bf16),
            pltpu.VMEM((hidden, width), bf16),
            blocks(zs),
            blocks(zs),
            blocks(zs),
            pltpu.VMEM((eight, 128), f32),
            pltpu.VMEM((eight, 128), f32),
            pltpu.VMEM((4 * zs, eight, width), bf16),
            pltpu.VMEM((count, hidden), f32),
            pltpu.VMEM((count, hidden), f32),
            pltpu.VMEM((count, hidden), bf16),
            pltpu.VMEM((7, 4 * zs, eight, half // 7), bf16),
            pltpu.VMEM((7, 4 * zs, eight, half // 7), bf16),
            pltpu.VMEM((7, 4 * zs, eight, half // 7), f32),
            blocks(2 * zs),
            blocks(2 * zs),
            blocks(zs),
            blocks(zs),
            blocks(zs),
            blocks(zs),
            pltpu.VMEM((eight, half), f32),
            pltpu.SemaphoreType.DMA((3,)),
        ]
        + sems(zs, zs)
        + one
        + sems(zs, zs, 2 * zs, 4 * zs, 7, 2 * zs, zs, zs)
        + one,
        compiler_params=pltpu.CompilerParams(
            collective_id=cid, has_side_effects=True, vmem_limit_bytes=60 * 1024 * 1024
        ),
    )(part, hid, gain, w_gate, w_up, w_down)


def _attend_kernel(tile, lengths, q_ref, new_ref, cache_ref, out_ref, top, denom, acc):
    b = pl.program_id(0)
    j = pl.program_id(1)
    f32 = jnp.float32
    scale = float(NOPE + ROPE) ** (-0.5)

    @pl.when(j == 0)
    def _():
        own = q_ref[0].astype(f32) * new_ref[0].astype(f32)
        top[...] = jnp.sum(own, axis=1, keepdims=True) * scale
        denom[...] = jnp.ones_like(denom)
        acc[...] = jnp.broadcast_to(new_ref[0][:, :KV_RANK].astype(f32), acc.shape)

    @pl.when(j * tile < lengths[b])
    def _():
        cache = cache_ref[0]
        scores = jnp.dot(q_ref[0], cache, preferred_element_type=f32) * scale
        positions = j * tile + lax.broadcasted_iota(jnp.int32, (1, tile), 1)
        scores = jnp.where(positions < lengths[b], scores, -jnp.inf)
        new_top = jnp.maximum(top[...], jnp.max(scores, axis=1, keepdims=True))
        weights = jnp.exp(scores - new_top)
        shrink = jnp.exp(top[...] - new_top)
        denom[...] = shrink * denom[...] + jnp.sum(weights, axis=1, keepdims=True)
        acc[...] = shrink * acc[...] + lax.dot_general(
            weights.astype(cache.dtype), cache[:KV_RANK], ROWS, preferred_element_type=f32
        )
        top[...] = new_top

    @pl.when(j == pl.num_programs(1) - 1)
    def _():
        result = (acc[...] / denom[...]).astype(out_ref.dtype)
        out_ref[:, 0] = result.reshape(out_ref.shape[0], out_ref.shape[2], out_ref.shape[3])


def attend(lengths, queries, new_kv, cache_kv, parts):
    seq_count, length, width = cache_kv.shape
    tile = length // 2
    heads = H // parts
    return pl.pallas_call(
        functools.partial(_attend_kernel, tile),
        out_shape=jax.ShapeDtypeStruct((parts, seq_count, heads, KV_RANK), queries.dtype),
        grid_spec=pltpu.PrefetchScalarGridSpec(
            num_scalar_prefetch=1,
            grid=(seq_count, 2),
            in_specs=[
                pl.BlockSpec((1, H, width), lambda b, j, n: (b, 0, 0)),
                pl.BlockSpec((1, 1, width), lambda b, j, n: (b, 0, 0)),
                pl.BlockSpec(
                    (1, width, tile),
                    lambda b, j, n: (b, 0, jnp.minimum(j, lax.div(n[b] - 1, tile))),
                ),
            ],
            out_specs=pl.BlockSpec((parts, 1, heads, KV_RANK), lambda b, j, n: (0, b, 0, 0)),
            scratch_shapes=[
                pltpu.VMEM((H, 1), jnp.float32),
                pltpu.VMEM((H, 1), jnp.float32),
                pltpu.VMEM((H, KV_RANK), jnp.float32),
            ],
        ),
        cost_estimate=pl.CostEstimate(
            flops=4 * seq_count * H * length * width,
            bytes_accessed=2 * cache_kv.size,
            transcendentals=seq_count * H * length,
        ),
    )(lengths, queries, new_kv.reshape(seq_count, 1, width), jnp.swapaxes(cache_kv, 1, 2))


def on_device(
    rep_count,
    group,
    hidden_in,
    q_nope,
    q_rope,
    new_kv,
    cache_kv,
    lengths,
    w_uk,
    w_uv,
    w_out,
    norm_gain,
    w_gate,
    w_up,
    w_down,
):
    seq_count = hidden_in.shape[0]
    heads_here = H // group
    slice_width = w_uk.shape[0]
    grp = lax.axis_index("grp")
    rep = lax.axis_index("rep")

    q_rows = exchange(q_nope.reshape(seq_count * H, NOPE), "rep", rep_count, True, 1)
    q_part = jnp.einsum(
        "bhd,chd->bhc",
        q_rows.reshape(rep_count * seq_count, H, NOPE),
        w_uk.reshape(slice_width, H, NOPE),
        preferred_element_type=jnp.float32,
    ).astype(jnp.bfloat16)
    q_back = exchange(
        q_part.reshape(rep_count, seq_count * H, slice_width), "rep", rep_count, False, 2
    )
    uv_own = lax.dynamic_slice_in_dim(w_uv, grp * heads_here * VH, heads_here * VH, 1)
    uv_own, q_back = lax.optimization_barrier((uv_own, q_back))
    uv_parts = jnp.zeros((rep_count,) + uv_own.shape, uv_own.dtype)
    uv_parts = lax.dynamic_update_slice_in_dim(uv_parts, uv_own[None], rep, 0)
    for step in range(1, rep_count):
        moved = lax.ppermute(
            uv_own, "rep", [(i, (i + step) % rep_count) for i in range(rep_count)]
        )
        source = lax.rem(rep + rep_count - step, rep_count)
        uv_parts = lax.dynamic_update_slice_in_dim(uv_parts, moved[None], source, 0)
    value_up = uv_parts.reshape(KV_RANK, heads_here, VH)

    q_lat = q_back.reshape(rep_count, seq_count, H, slice_width)
    queries = jnp.concatenate(
        [q_lat[i] for i in range(rep_count)] + [q_rope.reshape(seq_count, H, ROPE)], axis=2
    )
    if heads_here % 8 == 0:
        by_heads = attend(lengths, queries, new_kv, cache_kv, group)
    else:
        latent = attend(lengths, queries, new_kv, cache_kv, 1)
        by_heads = latent.reshape(seq_count, group, heads_here, KV_RANK).transpose(1, 0, 2, 3)
    latent_here = exchange(
        by_heads.reshape(group, seq_count * heads_here, KV_RANK), "grp", group, False, 3
    ).reshape(group * seq_count, heads_here, KV_RANK)
    head_out = jnp.einsum(
        "bhc,che->bhe", latent_here, value_up, preferred_element_type=jnp.float32
    ).astype(jnp.bfloat16)
    core = lax.rem(rep, 2)
    half = w_out.shape[1] // 2
    head_pair, hidden_pair = pair_gather(
        head_out.reshape(group * seq_count, heads_here * VH), hidden_in, 4
    )
    chip_rows = (
        head_pair.reshape(2, group, seq_count, -1)
        .transpose(1, 0, 2, 3)
        .reshape(group * 2 * seq_count, -1)
    )
    part = half_product(jnp.full((1,), core, jnp.int32), chip_rows, w_out)
    hid = lax.dynamic_slice_in_dim(hidden_pair.reshape(2 * seq_count, -1), core * half, half, 1)
    gain = lax.dynamic_slice_in_dim(norm_gain[None], core * half, half, 1)
    total = mlp_all(
        part.reshape(group, 2 * seq_count, half), hid, gain, w_gate.T, w_up.T, w_down, group, 5
    )
    return lax.dynamic_slice_in_dim(total, core * seq_count, seq_count, 0)


def solution(mesh):
    return jax.shard_map(
        functools.partial(on_device, mesh.shape["rep"], mesh.shape["grp"]),
        mesh=mesh,
        in_specs=(
            P(("rep", "grp"), None),
            P(("rep", "grp"), None),
            P(("rep", "grp"), None),
            P(("rep", "grp"), None),
            P(("rep", "grp"), None, None),
            P(("rep", "grp")),
            P("rep", None),
            P("rep", None),
            P("grp", None),
            P(),
            P(None, ("rep", "grp")),
            P(None, ("rep", "grp")),
            P(("rep", "grp"), None),
        ),
        out_specs=P(("rep", "grp"), None),
        check_vma=False,
    )
```
